32 devices in a mesh: group: 8 (over z, x), tensor: 4 (over y, core).
Axes of the slice: x: 2, y: 2, z: 4, core: 2. Of those that a mesh axis runs over, the one named last changes fastest.
Arguments:
- queries: bfloat16 [64, 64, 5120], P('group', None, 'tensor'), may hold values from -15 to 15
- prefix_keys: bfloat16 [16, 1024, 1024], P('group', None, 'tensor'), may hold values from -200 to 200
- prefix_values: bfloat16 [16, 1024, 1024], P('group', None, 'tensor'), may hold values from -6 to 6
- slot_of_prompt: int32 [16], replicated, may hold values from 0 to 15, as said below
- prompt_of: int32 [64], P('group'), may hold values from 0 to 15, as said below
- lengths: int32 [64], P('group'), may hold values from 1 to 64
Outputs:
- attended: bfloat16 [64, 64, 5120], P('group', 'tensor')
The draws below stay inside these ranges and needn't reach their ends.
Inputs may be any that keep to these rules, and one draw needn't show every extreme that they name: A permutation: prompt p's keys and values lie in row slot_of_prompt[p] of the prefix arrays, and that row belongs to group index slot_of_prompt[p] // 2. `prompt_of`: of the 8 completions on one group index, at most 2 have prompts cached on any one group index, and on every group index some group index caches the prompts of exactly 2 of them.
All inputs are finite; a program needn't handle non-finite values.
Results may differ from the reference program's by a relative error of at most 0.012.
Values may be sent and summed in bfloat16 or wider, within the bound.
A program may use at most 128 MiB of HBM per device.

```python
import math
import jax
import jax.numpy as jnp
from jax import lax

D = 5120
HEADS = 40
KV_HEADS = 8
HEAD = 128
PREFIX = 1024
COMP = 64
CAPC = 2
PPG = 2
CPD = 8
COMPLETIONS = 64
PROMPTS = 16


def routing_tables(key):
    base = jax.random.fold_in(key, 4217)
    first_key, second_key = jax.random.split(base, 2)
    slot_of_prompt = jax.random.permutation(first_key, PROMPTS).astype(jnp.int32)
    prompt_at = jnp.argsort(slot_of_prompt, stable=True).astype(jnp.int32)
    blocks = COMPLETIONS // CPD
    block_keys = jax.random.split(second_key, blocks)

    def one_block(block_key):
        key_spare, key_order, key_offset, key_local = jax.random.split(block_key, 4)
        spare = CAPC + jax.random.permutation(key_spare, blocks * CAPC - CAPC)
        chosen = jnp.concatenate([jnp.arange(CAPC), spare[:CPD - CAPC]])
        chosen = jax.random.permutation(key_order, chosen)
        offset = jax.random.randint(key_offset, (), 0, blocks)
        owner_group = (chosen // CAPC + offset) % blocks
        local_rows = jax.random.randint(key_local, (CPD,), 0, PPG)
        return owner_group * PPG + local_rows
    cache_slots = jax.vmap(one_block)(block_keys).reshape(COMPLETIONS)
    prompt_of = prompt_at[cache_slots].astype(jnp.int32)
    return (slot_of_prompt, prompt_of)


def draw_slot_of_prompt(key, part):
    return routing_tables(key)[0]


def draw_prompt_of(key, part):
    return routing_tables(key)[1]


def draw_prefix_keys(key, part):
    base = jax.random.fold_in(key, 913)
    key_base = jax.random.fold_in(base, 0)
    entries = jax.random.normal(key_base, (PROMPTS, PREFIX, KV_HEADS, HEAD), jnp.float32)
    entries = jnp.clip(entries, -200.0, 200.0)
    return entries.reshape(PROMPTS, PREFIX, KV_HEADS * HEAD).astype(jnp.bfloat16)


def place_ends(array, stream_key, smallest, largest):
    dims = array.shape
    spot = [jax.random.randint(jax.random.fold_in(stream_key, axis), (), 0, dims[axis]) for axis in range(len(dims))]
    array = array.at[tuple(spot)].set(smallest)
    longest = dims.index(max(dims))
    spot[longest] = (spot[longest] + 1) % dims[longest]
    return array.at[tuple(spot)].set(largest)


def shard_levels(stream_key, shape, cuts, smallest, largest):
    level = 1.0
    for position, blocks in cuts:
        draws = jax.random.uniform(jax.random.fold_in(jax.random.fold_in(stream_key, 6), position), (blocks,), jnp.float32, smallest / len(cuts), largest / len(cuts))
        level = level * jnp.repeat(jnp.exp(draws), shape[position] // blocks).reshape((-1,) + (1,) * (len(shape) - 1 - position))
    return level


def bell_draw(rng, shape, deviation, limit, pieces=(), kind=jnp.bfloat16):
    values = deviation * jax.random.normal(rng, shape, jnp.float32)
    if pieces:
        values = values * shard_levels(rng, shape, pieces, -0.22, 0.18)
    return jnp.clip(values, -limit, limit).astype(kind)


def setup_inputs(seed: int = 0) -> dict:
    key_list = jax.random.split(jax.random.key(seed), 7)
    queries = bell_draw(key_list[0], (COMPLETIONS, COMP, D), 2.5, 15.0, ((0, 8), (2, 4)))
    prefix_keys = draw_prefix_keys(jax.random.fold_in(key_list[6], 71), 0)
    prefix_values = bell_draw(key_list[2], (PROMPTS, PREFIX, KV_HEADS * HEAD), 1.0, 6.0, ((0, 8), (2, 4)))
    slot_of_prompt = draw_slot_of_prompt(jax.random.fold_in(key_list[6], 71), 0)
    prompt_of = draw_prompt_of(jax.random.fold_in(key_list[6], 71), 0)
    lengths = place_ends(jax.random.randint(key_list[5], (COMPLETIONS,), 1, COMP + 1), jax.random.fold_in(key_list[5], 1), 1, COMP).astype(jnp.int32)
    return dict(queries=queries, prefix_keys=prefix_keys, prefix_values=prefix_values, slot_of_prompt=slot_of_prompt, prompt_of=prompt_of, lengths=lengths)


rotary_base = 1000000.0

def rotary(head_rows, positions):
    half_dim = head_rows.shape[-1] // 2
    frequencies = rotary_base ** (-(jnp.arange(half_dim, dtype=jnp.float32) * 2.0 / head_rows.shape[-1]))
    angles = positions[:, None] * frequencies[None, :]
    cos_table = jnp.cos(angles)[:, None, :]
    sin_table = jnp.sin(angles)[:, None, :]
    first_half = head_rows[..., :half_dim]
    second_half = head_rows[..., half_dim:]
    return jnp.concatenate([first_half * cos_table - second_half * sin_table, second_half * cos_table + first_half * sin_table], axis=-1)

def reference(queries, prefix_keys, prefix_values, slot_of_prompt, prompt_of, lengths):
    positions = (PREFIX + jnp.arange(COMP)).astype(jnp.float32)
    cache_rows = slot_of_prompt[prompt_of].astype(jnp.int32)
    per_kv = HEADS // KV_HEADS
    scaling = 1.0 / math.sqrt(HEAD)
    highest = lax.Precision.HIGHEST

    def single(inputs):
        query_rows, cache_row, length = inputs
        roped = rotary(query_rows.astype(jnp.float32).reshape(COMP, HEADS, HEAD), positions).astype(jnp.bfloat16)
        grouped = roped.astype(jnp.float32).reshape(COMP, KV_HEADS, per_kv, HEAD)
        cached_keys = lax.dynamic_index_in_dim(prefix_keys, cache_row, 0, keepdims=False).astype(jnp.float32).reshape(PREFIX, KV_HEADS, HEAD)
        cached_values = lax.dynamic_index_in_dim(prefix_values, cache_row, 0, keepdims=False).astype(jnp.float32).reshape(PREFIX, KV_HEADS, HEAD)
        scores = jnp.einsum('rkgd,pkd->kgrp', grouped, cached_keys, precision=highest) * scaling
        peak = lax.optimization_barrier(jnp.max(scores, axis=-1, keepdims=True))
        weights = jnp.exp(scores - peak)
        denominator = lax.optimization_barrier(jnp.sum(weights, axis=-1))
        probabilities = weights.astype(jnp.bfloat16).astype(jnp.float32)
        weighted = jnp.einsum('kgrp,pkd->rkgd', probabilities, cached_values, precision=highest)
        attended = (weighted / jnp.transpose(denominator, (2, 0, 1))[..., None]).astype(jnp.bfloat16).reshape(COMP, D)
        live_rows = jnp.arange(COMP) < length
        return jnp.where(live_rows[:, None], attended, jnp.zeros_like(attended))
    return lax.map(single, (queries, cache_rows, lengths))
```

```python
import functools
import math

import numpy as np

import jax
import jax.numpy as jnp
from jax import lax
from jax.experimental import pallas as pl
from jax.experimental.pallas import tpu as pltpu
from jax.sharding import PartitionSpec as P

HEAD = 128
CAPC = 2
ROTARY_BASE = 1000000.0
TILE = 16
MESH = pl.DeviceIdType.MESH


def rotary_tables(first_position, rows):
    half = HEAD // 2
    frequencies = np.float32(ROTARY_BASE) ** (
        -(np.arange(half, dtype=np.float32) * np.float32(2.0) / np.float32(HEAD))
    )
    positions = (first_position + np.arange(rows)).astype(np.float32)
    angles = (positions[:, None] * frequencies.astype(np.float32)[None, :]).astype(np.float64)
    cos, sin = np.cos(angles), np.sin(angles)
    return (
        np.concatenate([cos, cos], axis=1).astype(np.float32),
        np.concatenate([-sin, sin], axis=1).astype(np.float32),
    )


def kernel(
    groups, lanes,
    source_ref, tag_ref, dest_ref, length_ref,
    q_ref, k_ref, v_ref, cos_ref, sin_ref,
    out_ref,
    q_out, q_in, sel_out, sel_in, res, stage,
    q_send, q_recv, s_send, s_recv, r_send, r_recv,
):
    me, lane = lax.axis_index("group"), lax.axis_index("tensor")
    held, rows, width = q_ref.shape
    cached, prefix, kv_width = k_ref.shape
    share = rows // lanes
    kv_local = kv_width // HEAD
    per_kv = width // HEAD // kv_local
    half = groups // 2
    factor = math.log2(math.e) / math.sqrt(HEAD)

    barrier = pltpu.get_barrier_semaphore()

    def greet(step, carry):
        for turn in range(lanes):
            def send():
                pl.semaphore_signal(
                    barrier, inc=1,
                    device_id=(lax.rem(me + step, groups), lax.rem(lane + turn, lanes)),
                    device_id_type=MESH,
                )
            if turn:
                send()
            else:
                pl.when(step > 0)(send)
        return carry

    lax.fori_loop(0, groups, greet, 0)

    def offset_of(step):
        swing = (step + 1) // 2
        return lax.rem(half + (1 - 2 * lax.rem(step, 2)) * swing + groups, groups)

    def prepare(owner, q_to, sel_to):
        for slot in range(CAPC):
            place = owner * CAPC + slot
            item = source_ref[place]
            tag = tag_ref[place]
            for j in range(cached):
                weight = jnp.where(tag == j, 1.0, 0.0)
                sel_to[owner, slot * cached + j] = jnp.full(
                    (TILE, HEAD), weight, jnp.float32
                ).astype(jnp.bfloat16)
            for head in range(width // HEAD):
                span = slice(head * HEAD, (head + 1) * HEAD)
                x = q_ref[item, :, span].astype(jnp.float32)
                turned = x * cos_ref[...] + pltpu.roll(x, HEAD // 2, 1) * sin_ref[...]
                q_to[owner, slot, :, span] = turned.astype(jnp.bfloat16)

    def q_copy(here, there, device):
        return pltpu.make_async_remote_copy(
            src_ref=q_out.at[here], dst_ref=q_in.at[there],
            send_sem=q_send.at[here], recv_sem=q_recv.at[there],
            device_id=(device, lane), device_id_type=MESH,
        )

    def s_copy(here, there, device):
        return pltpu.make_async_remote_copy(
            src_ref=sel_out.at[here], dst_ref=sel_in.at[there],
            send_sem=s_send.at[here], recv_sem=s_recv.at[there],
            device_id=(device, lane), device_id_type=MESH,
        )

    def r_copy(item, piece, owner, from_lane, device):
        return pltpu.make_async_remote_copy(
            src_ref=res.at[item, :, piece],
            dst_ref=stage.at[
                pl.ds(owner * CAPC, CAPC), :,
                pl.ds(pl.multiple_of(from_lane * width, HEAD), width),
            ],
            send_sem=r_send.at[item, piece], recv_sem=r_recv.at[owner, from_lane],
            device_id=device, device_id_type=MESH,
        )

    def dispatch(step, carry):
        owner = lax.rem(me + offset_of(step), groups)
        prepare(owner, q_out, sel_out)

        @pl.when(step == 0)
        def _():
            pl.semaphore_wait(barrier, groups * lanes - 1)

        s_copy(owner, me, owner).start()
        q_copy(owner, me, owner).start()
        return carry

    lax.fori_loop(0, groups - 1, dispatch, 0)
    prepare(me, q_in, sel_in)

    def attend(source, slot):
        weights = [sel_in[source, slot * cached + j][None] for j in range(cached)]

        def chosen(ref, span):
            total = None
            for j in range(cached):
                part = ref[j, :, span].reshape(prefix // TILE, TILE, HEAD) * weights[j]
                total = part if total is None else total + part
            return total.reshape(prefix, HEAD)

        for kv in range(kv_local):
            span = slice(kv * HEAD, (kv + 1) * HEAD)
            spans = [
                slice((kv * per_kv + g) * HEAD, (kv * per_kv + g + 1) * HEAD)
                for g in range(per_kv)
            ]
            query = jnp.concatenate([q_in[source, slot, :, s] for s in spans], axis=0)
            scores = lax.dot_general(
                query, chosen(k_ref, span), (((1,), (1,)), ((), ())),
                preferred_element_type=jnp.float32,
            )
            peak = jnp.max(scores, axis=-1, keepdims=True)
            weight = jnp.exp2((scores - peak) * factor)
            total = jnp.sum(weight, axis=-1, keepdims=True)
            mixed = jnp.dot(
                weight.astype(jnp.bfloat16), chosen(v_ref, span),
                preferred_element_type=jnp.float32,
            )
            mixed = (mixed / total).astype(jnp.bfloat16)
            for g in range(per_kv):
                res[source, slot, :, :, spans[g]] = mixed[g * rows:(g + 1) * rows].reshape(
                    lanes, share, HEAD
                )

    def work(step, carry):
        source = lax.rem(me + groups - offset_of(lax.rem(step + groups - 1, groups)), groups)

        @pl.when(step > 0)
        def _():
            s_copy(source, source, source).wait_recv()
            q_copy(source, source, source).wait_recv()

        for slot in range(CAPC):
            attend(source, slot)
        for turn in range(1, lanes):
            piece = lax.rem(lane + turn, lanes)
            r_copy(source, piece, me, lane, (source, piece)).start()

        @pl.when(step > 0)
        def _():
            r_copy(source, lane, me, lane, (source, lane)).start()

        @pl.when(step == 0)
        def _():
            stage[
                pl.ds(me * CAPC, CAPC), :,
                pl.ds(pl.multiple_of(lane * width, HEAD), width),
            ] = res[source, :, lane]

        return carry

    lax.fori_loop(0, groups, work, 0)

    def settle(step, carry):
        other = lax.rem(me + step, groups)

        @pl.when(step > 0)
        def _():
            s_copy(other, me, other).wait_send()
            q_copy(other, me, other).wait_send()
            r_copy(other, lane, other, lane, (other, lane)).wait_send()
            r_copy(other, lane, other, lane, (other, lane)).wait_recv()

        for turn in range(1, lanes):
            piece = lax.rem(lane + turn, lanes)
            r_copy(other, piece, other, piece, (other, piece)).wait_send()
            r_copy(other, piece, other, piece, (other, piece)).wait_recv()
        return carry

    lax.fori_loop(0, groups, settle, 0)

    def deliver(item, carry):
        found = stage[dest_ref[item]].astype(jnp.float32)
        position = lane * share + lax.broadcasted_iota(jnp.int32, found.shape, 0)
        out_ref[item] = jnp.where(position < length_ref[item], found, 0.0).astype(jnp.bfloat16)
        return carry

    lax.fori_loop(0, held, deliver, 0)


def local(groups, lanes, queries, prefix_keys, prefix_values, slot_of_prompt, prompt_of, lengths):
    held, rows, width = queries.shape
    cached, prefix, kv_width = prefix_keys.shape
    share = rows // lanes
    cos, sin = rotary_tables(prefix, rows)
    cache_rows = slot_of_prompt[prompt_of]
    owner = cache_rows // cached
    serial = jnp.arange(held)
    earlier = (owner[None, :] == owner[:, None]) & (serial[None, :] < serial[:, None])
    destination = owner * CAPC + jnp.sum(earlier.astype(jnp.int32), axis=1)
    matches = destination[None, :] == jnp.arange(groups * CAPC)[:, None]
    source = jnp.sum(jnp.where(matches, serial[None, :], 0), axis=1)
    tags = jnp.sum(jnp.where(matches, (cache_rows % cached)[None, :], 0), axis=1)
    smem = pl.BlockSpec(memory_space=pltpu.SMEM)
    vmem = pl.BlockSpec(memory_space=pltpu.VMEM)
    dma = pltpu.SemaphoreType.DMA
    bf16 = jnp.bfloat16
    return pl.pallas_call(
        functools.partial(kernel, groups, lanes),
        out_shape=jax.ShapeDtypeStruct((held, share, width * lanes), bf16),
        in_specs=[smem] * 4 + [vmem] * 5,
        out_specs=vmem,
        scratch_shapes=[
            pltpu.VMEM((groups, CAPC, rows, width), bf16),
            pltpu.VMEM((groups, CAPC, rows, width), bf16),
            pltpu.VMEM((groups, CAPC * cached, TILE, HEAD), bf16),
            pltpu.VMEM((groups, CAPC * cached, TILE, HEAD), bf16),
            pltpu.VMEM((groups, CAPC, lanes, share, width), bf16),
            pltpu.VMEM((groups * CAPC, share, width * lanes), bf16),
            dma((groups,)), dma((groups,)),
            dma((groups,)), dma((groups,)),
            dma((groups, lanes)), dma((groups, lanes)),
        ],
        compiler_params=pltpu.CompilerParams(collective_id=0, has_side_effects=True),
        name="routed_prefix_attention",
    )(
        source.astype(jnp.int32), tags.astype(jnp.int32), destination.astype(jnp.int32), lengths,
        queries, prefix_keys, prefix_values, jnp.asarray(cos), jnp.asarray(sin),
    )


def solution(mesh):
    placed = (
        P("group", None, "tensor"),
        P("group", None, "tensor"),
        P("group", None, "tensor"),
        P(),
        P("group"),
        P("group"),
    )
    return jax.shard_map(
        functools.partial(local, mesh.shape["group"], mesh.shape["tensor"]),
        mesh=mesh, in_specs=placed, out_specs=P("group", "tensor", None), check_vma=False,
    )
```
